32 devices in a mesh: feat: 4 (over y, x), dp: 8 (over z, core).
Axes of the slice: x: 2, y: 2, z: 4, core: 2. Of those that a mesh axis runs over, the one named last changes fastest.
Arguments:
- layer_inputs: bfloat16 [4, 24, 128, 5120], P('feat', 'dp'), may hold values from -6 to 6
- output_grads: bfloat16 [4, 24, 128, 5120], P('feat', 'dp'), may hold values from -6 to 6
- adapter_a: bfloat16 [4, 128, 5120], P('feat'), may hold values from -0.078125 to 0.078125
- adapter_b: bfloat16 [4, 5120, 128], P('feat'), may hold values from -0.5 to 0.5
- out_factor: bfloat16 [4, 5120, 64], P('feat'), may hold values from -0.5 to 0.5
- in_factor: bfloat16 [4, 5120, 64], P('feat'), may hold values from -0.5 to 0.5
- rank_factor_b: bfloat16 [4, 128, 128], P('feat'), may hold values from -0.5 to 0.5
- rank_factor_a: bfloat16 [4, 128, 128], P('feat'), may hold values from -0.5 to 0.5
- token_counts: int32 [24], P('dp'), may hold values from 16 to 128, as said below
- val_grads: bfloat16 [256, 8192], P('dp', 'feat'), may hold values from -40 to 40
- val_domain: int32 [256, 1], P('dp'), may hold values from 0 to 7
Outputs:
- train_features: bfloat16 [24, 8192], P('dp', 'feat')
- domain_scores: float32 [24, 8], P('dp')
The draws below stay inside these ranges and needn't reach their ends.
Inputs may be any that keep to these rules, and one draw needn't show every extreme that they name: `token_counts`: some example has all 128 positions live; positions at or past an example's count are padding.
All inputs are finite; a program needn't handle non-finite values.
Results may differ from the reference program's by a relative error of at most 0.0064.
Values may be sent and summed in bfloat16 or wider, within the bound.
No kernel may reach another device: no remote copies, remote signals or barrier semaphores. Data moves between devices by JAX's collectives and lax.ppermute only.
A program may use at most 64 MiB of HBM per device.

```python
import math
import jax
import jax.numpy as jnp
from jax import lax

D = 5120
R = 128
K1 = 64
K2 = 128
PROJ = 8192
DOMAINS = 8
ADAPTERS = 4
SEQ = 128
TRAIN = 24
VAL = 256


def factor_draw(key):
    key_base, key_scale = jax.random.split(key)
    scales = jnp.exp(jax.random.uniform(key_scale, (ADAPTERS, 1, K1), jnp.float32) * math.log(10.0)) / math.sqrt(10.0)
    base = jax.random.normal(key_base, (ADAPTERS, D, K1), jnp.float32)
    return jnp.clip(base * scales / math.sqrt(D), -0.5, 0.5).astype(jnp.bfloat16)


def draw_out_factor(key, part):
    return factor_draw(jax.random.fold_in(key, 11))


def draw_in_factor(key, part):
    return factor_draw(jax.random.fold_in(key, 12))


def draw_token_counts(key, part):
    key_counts, key_full = jax.random.split(jax.random.fold_in(key, 13))
    counts = jax.random.randint(key_counts, (TRAIN,), max(1, SEQ // 8), SEQ + 1, jnp.int32)
    full_row = jax.random.randint(key_full, (), 0, TRAIN, jnp.int32)
    return jnp.where(jnp.arange(TRAIN, dtype=jnp.int32) == full_row, SEQ, counts).astype(jnp.int32)


def draw_val_grads(key, part):
    key_base, key_rows, key_cols = jax.random.split(jax.random.fold_in(key, 14), 3)
    half_log = 0.5 * math.log(10.0)
    row_scale = jnp.exp(jax.random.uniform(key_rows, (VAL, 1), jnp.float32) * half_log)
    col_scale = jnp.exp(jax.random.uniform(key_cols, (1, PROJ), jnp.float32) * half_log)
    base = jax.random.normal(key_base, (VAL, PROJ), jnp.float32)
    return jnp.clip(base * row_scale * col_scale, -40.0, 40.0).astype(jnp.bfloat16)


def block_scale(key, extent, pieces, low, largest):
    def one(dim, parts):
        heights = jax.random.uniform(jax.random.fold_in(jax.random.fold_in(key, 6), dim), (parts,), jnp.float32, low / len(pieces), largest / len(pieces))
        return jnp.repeat(jnp.exp(heights), extent[dim] // parts).reshape((-1,) + (1,) * (len(extent) - dim - 1))

    factor_of = one(*pieces[0])
    for cut in pieces[1:]:
        factor_of = factor_of * one(*cut)
    return factor_of


def different_ones(stream_key, rows, count, top, lift):
    order = jax.random.permutation(jax.random.fold_in(stream_key, 1), count)
    boost = order
    for power in range(3):
        boost = boost * boost // count
    boost = boost * lift // count
    chance = jax.random.randint(jax.random.fold_in(stream_key, 2), (rows, count), 0, 4096) + boost
    sure = jax.random.permutation(jax.random.fold_in(stream_key, 3), rows)[jnp.arange(count) % rows]
    chance = jnp.where(jnp.arange(rows)[:, None] == sure[None, :], 1 << 14, chance)
    merit = chance * count + jnp.arange(count)
    return lax.top_k(merit.astype(jnp.int32), top)[1].astype(jnp.int32)


def scatter_about(key, shape, width, reach, pieces=(), held_as=jnp.bfloat16):
    values = width * jax.random.normal(key, shape, jnp.float32)
    if pieces:
        values = values * block_scale(key, shape, pieces, -0.22, 0.18)
    return jnp.clip(values, -reach, reach).astype(held_as)


def setup_inputs(seed: int = 0) -> dict:
    key_of = jax.random.split(jax.random.key(seed), 12)
    return {
        "layer_inputs": scatter_about(key_of[0], (ADAPTERS, TRAIN, SEQ, D), 1.0, 6.0, ((0, 4), (1, 8))),
        "output_grads": scatter_about(key_of[1], (ADAPTERS, TRAIN, SEQ, D), 1.0, 6.0, ((0, 4), (1, 8))),
        "adapter_a": scatter_about(key_of[2], (ADAPTERS, R, D), D ** -0.5, 0.078125, ((0, 4),)),
        "adapter_b": scatter_about(key_of[3], (ADAPTERS, D, R), R ** -0.5, 0.5, ((0, 4),)),
        "out_factor": draw_out_factor(jax.random.fold_in(key_of[11], 71), 0),
        "in_factor": draw_in_factor(jax.random.fold_in(key_of[11], 71), 0),
        "rank_factor_b": scatter_about(key_of[6], (ADAPTERS, R, K2), R ** -0.5, 0.5, ((0, 4),)),
        "rank_factor_a": scatter_about(key_of[7], (ADAPTERS, R, K2), R ** -0.5, 0.5, ((0, 4),)),
        "token_counts": draw_token_counts(jax.random.fold_in(key_of[11], 71), 0),
        "val_grads": draw_val_grads(jax.random.fold_in(key_of[11], 71), 0),
        "val_domain": different_ones(key_of[10], VAL, DOMAINS, 1, 2048),
    }


norm_eps = 1e-06

def adapter_term(inputs_two, grads_two, weight_a, weight_b, factor_out, factor_in, rank_b, rank_a, both_mask):
    hidden = jnp.dot(inputs_two, weight_a.T, preferred_element_type=jnp.float32).astype(jnp.bfloat16)
    input_proj = jnp.dot(inputs_two, factor_in, preferred_element_type=jnp.float32).astype(jnp.bfloat16)
    backward = jnp.dot(grads_two, weight_b, preferred_element_type=jnp.float32).astype(jnp.bfloat16)
    grad_proj = jnp.dot(grads_two, factor_out, preferred_element_type=jnp.float32).astype(jnp.bfloat16)
    hidden_rank = jnp.dot(hidden, rank_b, preferred_element_type=jnp.float32).astype(jnp.bfloat16)
    back_rank = jnp.dot(backward, rank_a, preferred_element_type=jnp.float32).astype(jnp.bfloat16)
    left_side = jnp.concatenate([grad_proj.reshape(TRAIN, SEQ, K1), input_proj.reshape(TRAIN, SEQ, K1)], axis=1)
    right_side = jnp.concatenate([hidden_rank.reshape(TRAIN, SEQ, K2), back_rank.reshape(TRAIN, SEQ, K2)], axis=1)
    left_side = jnp.where(both_mask, left_side, jnp.zeros_like(left_side))
    return jnp.einsum('etk,etj->ekj', left_side.astype(jnp.float32), right_side.astype(jnp.float32))

def reference(layer_inputs, output_grads, adapter_a, adapter_b, out_factor, in_factor, rank_factor_b, rank_factor_a, token_counts, val_grads, val_domain):
    positions = jnp.arange(SEQ, dtype=jnp.int32)
    live_mask = positions[None, :] < token_counts[:, None]
    both_mask = jnp.concatenate([live_mask, live_mask], axis=1)[:, :, None]
    summed = jnp.zeros((TRAIN, K1, K2), jnp.float32)
    for which in range(ADAPTERS):
        summed = summed + adapter_term(layer_inputs[which].reshape(TRAIN * SEQ, D), output_grads[which].reshape(TRAIN * SEQ, D), adapter_a[which], adapter_b[which], out_factor[which], in_factor[which], rank_factor_b[which], rank_factor_a[which], both_mask)
    counts_float = token_counts.astype(jnp.float32)
    train_features = (summed.reshape(TRAIN, PROJ) / counts_float[:, None]).astype(jnp.bfloat16)
    train_float = train_features.astype(jnp.float32)
    val_float = val_grads.astype(jnp.float32)
    train_norm = lax.optimization_barrier(jnp.sum(train_float * train_float, axis=1))
    val_norm = lax.optimization_barrier(jnp.sum(val_float * val_float, axis=1))
    inner = jnp.dot(train_features, val_grads.T, preferred_element_type=jnp.float32)
    cosine = inner * lax.rsqrt(train_norm + norm_eps)[:, None] * lax.rsqrt(val_norm + norm_eps)[None, :]
    onehot = (val_domain == jnp.arange(DOMAINS, dtype=jnp.int32)[None, :]).astype(jnp.float32)
    domain_sizes = lax.optimization_barrier(jnp.sum(onehot, axis=0))
    totals = jnp.dot(cosine, onehot, precision=lax.Precision.HIGHEST)
    domain_scores = math.sqrt(PROJ) * totals / domain_sizes[None, :]
    return (train_features, domain_scores)
```

```python
import functools
import math

import jax
import jax.numpy as jnp
from jax import lax
from jax.experimental import pallas as pl
from jax.experimental.pallas import tpu as pltpu
from jax.sharding import PartitionSpec as P

PROJ = 8192
DOMAINS = 8
LANES = 128

norm_eps = 1e-06

NT = (((1,), (1,)), ((), ()))
NN = (((1,), (0,)), ((), ()))
TN = (((0,), (0,)), ((), ()))


def dot32(left, right, dims, precision=None):
    return lax.dot_general(
        left, right, dims, precision=precision, preferred_element_type=jnp.float32
    )


def project_kernel(
    feat_size,
    steps,
    index_ref,
    counts_ref,
    x_ref,
    g_ref,
    a_ref,
    b_ref,
    of_ref,
    if_ref,
    rb_ref,
    ra_ref,
    *rest,
):
    outs = rest[:feat_size]
    acc_x, acc_b, acc_o, terms = rest[feat_size:]
    step = pl.program_id(0)
    rank = a_ref.shape[0]
    rows = of_ref.shape[0]
    examples = terms.shape[0]
    seq = acc_x.shape[0] // examples

    @pl.when(step == 0)
    def _():
        acc_x[...] = jnp.zeros_like(acc_x)
        acc_b[...] = jnp.zeros_like(acc_b)
        acc_o[...] = jnp.zeros_like(acc_o)

    weights_x = jnp.concatenate([a_ref[...], if_ref[...]], axis=0)
    acc_x[...] += dot32(x_ref[...], weights_x, NT)
    acc_b[...] += dot32(g_ref[...], b_ref[...], NN)
    acc_o[...] += dot32(g_ref[...], of_ref[...], NT)

    @pl.when(step == steps - 1)
    def _():
        hidden = acc_x[:, :rank].astype(jnp.bfloat16)
        back = acc_b[...].astype(jnp.bfloat16)
        hidden_rank = dot32(hidden, rb_ref[...], NN).astype(jnp.bfloat16)
        back_rank = dot32(back, ra_ref[...], NN).astype(jnp.bfloat16)
        place = lax.broadcasted_iota(jnp.int32, (seq, rows), 0)
        for e in range(examples):
            span = slice(e * seq, (e + 1) * seq)
            live = place < counts_ref[e]
            gp = jnp.where(live, acc_o[span, :], 0.0).astype(jnp.bfloat16)
            ip = jnp.where(live, acc_x[span, rank:], 0.0).astype(jnp.bfloat16)
            terms[e] = dot32(gp, hidden_rank[span], TN) + dot32(ip, back_rank[span], TN)
        part = rows // feat_size
        here = index_ref[0]
        for s in range(feat_size):
            owner = lax.rem(here + s, feat_size)
            start = pl.multiple_of(owner * part, part)
            outs[s][...] = terms[:, pl.ds(start, part), :]


def project(index, counts, x, g, a, b, of_t, if_t, rb, ra, feat_size, examples):
    tokens, width = x.shape
    rank = a.shape[0]
    rows = of_t.shape[0]
    cols = rb.shape[1]
    steps = 10
    kb = width // steps
    part = rows // feat_size
    smem = pl.BlockSpec(memory_space=pltpu.SMEM)
    whole = lambda shape: pl.BlockSpec(shape, lambda k: (0,) * len(shape))
    return pl.pallas_call(
        functools.partial(project_kernel, feat_size, steps),
        grid=(steps,),
        in_specs=[
            smem,
            smem,
            pl.BlockSpec((tokens, kb), lambda k: (0, k)),
            pl.BlockSpec((tokens, kb), lambda k: (0, k)),
            pl.BlockSpec((rank, kb), lambda k: (0, k)),
            pl.BlockSpec((kb, rank), lambda k: (k, 0)),
            pl.BlockSpec((rows, kb), lambda k: (0, k)),
            pl.BlockSpec((rows, kb), lambda k: (0, k)),
            whole(rb.shape),
            whole(ra.shape),
        ],
        out_specs=[whole((examples, part, cols))] * feat_size,
        out_shape=[jax.ShapeDtypeStruct((examples, part, cols), jnp.float32)] * feat_size,
        scratch_shapes=[
            pltpu.VMEM((tokens, rank + rows), jnp.float32),
            pltpu.VMEM((tokens, rank), jnp.float32),
            pltpu.VMEM((tokens, rows), jnp.float32),
            pltpu.VMEM((examples, rows, cols), jnp.float32),
        ],
        cost_estimate=pl.CostEstimate(
            flops=4 * tokens * width * (rank + rows),
            bytes_accessed=2 * (2 * tokens + 2 * rank + 2 * rows) * width,
            transcendentals=0,
        ),
        compiler_params=pltpu.CompilerParams(dimension_semantics=("arbitrary",)),
        name="project",
    )(index, counts, x, g, a, b, of_t, if_t, rb, ra)


def norms_kernel(near_ref, far_ref, out_ref):
    width = near_ref.shape[1] - LANES
    half = near_ref.shape[0]
    ones = jnp.ones((8, LANES), jnp.float32)
    for which, ref in enumerate((near_ref, far_ref)):
        total = jnp.zeros((half, LANES), jnp.float32)
        for c in range(0, width, LANES):
            piece = ref[:, c : c + LANES].astype(jnp.float32)
            total = total + piece * piece
        out_ref[:, which * half : (which + 1) * half] = dot32(
            ones, total, NT, lax.Precision.HIGHEST
        )


def combine_kernel(feat_size, counts_ref, *rest):
    blocks = rest[:feat_size]
    near_ref, far_ref, norms_ref, feat_ref, pack_ref, flat = rest[feat_size:]
    summed = blocks[0][...]
    for ref in blocks[1:]:
        summed = summed + ref[...]
    examples, part, cols = summed.shape
    half = near_ref.shape[0]
    pack_ref[...] = jnp.zeros_like(pack_ref)
    flat[...] = jnp.zeros_like(flat)
    for e in range(examples):
        value = (summed[e] / counts_ref[e].astype(jnp.float32)).astype(jnp.bfloat16)
        value = value.astype(jnp.float32)
        for k in range(part):
            flat[e : e + 1, k * cols : (k + 1) * cols] = value[k : k + 1, :]
    flat_value = flat[...]
    features = flat_value.astype(jnp.bfloat16)
    feat_ref[...] = features[:examples]
    norm = jnp.sum(flat_value * flat_value, axis=1, keepdims=True)
    width = part * cols
    inner_near = dot32(features, near_ref[:, :width], NT)
    inner_far = dot32(features, far_ref[:, :width], NT)
    pack_ref[:8, :half] = inner_near
    pack_ref[:8, half:] = inner_far
    pack_ref[8:16, :] = norms_ref[...]
    pack_ref[16:24, :] = jnp.broadcast_to(norm, pack_ref[16:24, :].shape)


def score_kernel(feat_size, scale, *rest):
    packs = rest[:feat_size]
    near_ref, far_ref, out_ref = rest[feat_size:]
    total = packs[0][...]
    for ref in packs[1:]:
        total = total + ref[...]
    half = near_ref.shape[0]
    examples = out_ref.shape[0]
    cosine = (
        total[:8]
        * lax.rsqrt(total[16:24] + norm_eps)
        * lax.rsqrt(total[8:16] + norm_eps)
    )
    ones = jnp.ones((8, half), jnp.float32)
    sums = jnp.zeros((8, LANES), jnp.float32)
    sizes = jnp.zeros((8, LANES), jnp.float32)
    for which, ref in enumerate((near_ref, far_ref)):
        ids = ref[...].astype(jnp.float32)
        lane = lax.broadcasted_iota(jnp.int32, ids.shape, 1).astype(jnp.float32)
        marks = jnp.where(ids == lane, 1.0, 0.0)
        piece = cosine[:, which * half : (which + 1) * half]
        sums = sums + dot32(piece, marks, NN, lax.Precision.HIGHEST)
        sizes = sizes + dot32(ones, marks, NN)
    out_ref[...] = (scale * sums / sizes)[:examples, : out_ref.shape[1]]


def shifted(value, axis, size, shift, stride=1):
    pairs = []
    for i in range(size):
        chip, core = divmod(i, stride)
        chips = size // stride
        pairs.append((i, ((chip + shift) % chips) * stride + core))
    return lax.ppermute(value, axis, pairs)


def local(
    feat_size,
    dp_size,
    layer_inputs,
    output_grads,
    adapter_a,
    adapter_b,
    out_factor,
    in_factor,
    rank_factor_b,
    rank_factor_a,
    token_counts,
    val_grads,
    val_domain,
):
    _, examples, seq_len, width = layer_inputs.shape
    val_rows, val_cols = val_grads.shape
    ids = jnp.broadcast_to(val_domain.astype(jnp.bfloat16), (val_rows, LANES))
    payload = jnp.concatenate([val_grads, ids], axis=1)
    chips = dp_size // 2
    pieces = [payload]
    for s in range(1, chips):
        pieces.append(shifted(payload, "dp", dp_size, s, 2))
    near = jnp.concatenate(pieces, axis=0)
    far = lax.ppermute(near, "dp", [(i, i ^ 1) for i in range(dp_size)])

    index = lax.axis_index("feat").astype(jnp.int32).reshape(1)
    blocks = project(
        index,
        token_counts,
        layer_inputs.reshape(examples * seq_len, width),
        output_grads.reshape(examples * seq_len, width),
        adapter_a[0],
        adapter_b[0],
        out_factor[0].T,
        in_factor[0].T,
        rank_factor_b[0],
        rank_factor_a[0],
        feat_size,
        examples,
    )
    held = [blocks[0]]
    for s in range(1, feat_size):
        held.append(shifted(blocks[s], "feat", feat_size, s))

    total_rows = 2 * near.shape[0]
    norms = pl.pallas_call(
        norms_kernel,
        out_shape=jax.ShapeDtypeStruct((8, total_rows), jnp.float32),
        name="norms",
    )(near, far)
    smem = pl.BlockSpec(memory_space=pltpu.SMEM)
    vmem = pl.BlockSpec(memory_space=pltpu.VMEM)
    train_features, pack = pl.pallas_call(
        functools.partial(combine_kernel, feat_size),
        in_specs=[smem] + [vmem] * (feat_size + 3),
        out_shape=[
            jax.ShapeDtypeStruct((examples, val_cols), jnp.bfloat16),
            jax.ShapeDtypeStruct((24, total_rows), jnp.float32),
        ],
        scratch_shapes=[pltpu.VMEM((8, val_cols), jnp.float32)],
        name="combine",
    )(token_counts, *held, near, far, norms)

    packs = [pack]
    for s in range(1, feat_size):
        packs.append(shifted(pack, "feat", feat_size, s))
    tail = pl.BlockSpec((near.shape[0], LANES), lambda i: (0, val_cols // LANES))
    whole = pl.BlockSpec(pack.shape, lambda i: (0, 0))
    domain_scores = pl.pallas_call(
        functools.partial(score_kernel, feat_size, math.sqrt(PROJ)),
        grid=(1,),
        in_specs=[whole] * feat_size + [tail, tail],
        out_specs=pl.BlockSpec((examples, DOMAINS), lambda i: (0, 0)),
        out_shape=jax.ShapeDtypeStruct((examples, DOMAINS), jnp.float32),
        name="score",
    )(*packs, near, far)
    return (train_features, domain_scores)


def solution(mesh):
    in_specs = (
        P("feat", "dp", None, None),
        P("feat", "dp", None, None),
        P("feat", None, None),
        P("feat", None, None),
        P("feat", None, None),
        P("feat", None, None),
        P("feat", None, None),
        P("feat", None, None),
        P("dp"),
        P("dp", "feat"),
        P("dp", None),
    )
    out_specs = (P("dp", "feat"), P("dp", None))
    body = functools.partial(local, mesh.shape["feat"], mesh.shape["dp"])
    return jax.shard_map(body, mesh=mesh, in_specs=in_specs, out_specs=out_specs, check_vma=False)
```

```python
import functools
import math

import jax
import jax.numpy as jnp
from jax import lax
from jax.experimental import pallas as pl
from jax.experimental.pallas import tpu as pltpu
from jax.sharding import Mesh
from jax.sharding import PartitionSpec as P

PROJ = 8192
DOMAINS = 8
LANES = 128
SUBLANES = 8

FAR = ("hi",)
NEAR = ("lo", "core")
DP = ("hi", "lo", "core")

norm_eps = 1e-06

NT = (((1,), (1,)), ((), ()))
NN = (((1,), (0,)), ((), ()))
TN = (((0,), (0,)), ((), ()))
HIGHEST = lax.Precision.HIGHEST


def dot32(left, right, dims, precision=None):
    return lax.dot_general(
        left, right, dims, precision=precision, preferred_element_type=jnp.float32
    )


def limit(mib):
    return pltpu.CompilerParams(vmem_limit_bytes=mib << 20)


def round_up(value, unit):
    return (value + unit - 1) // unit * unit


def payload_kernel(val_ref, domain_ref, out_ref):
    rows = val_ref.shape[0]
    out_ref[:rows, :] = val_ref[...]
    out_ref[rows:, :] = jnp.zeros_like(out_ref[rows:, :])
    ids = jnp.broadcast_to(domain_ref[...].astype(jnp.float32), (SUBLANES, rows))
    out_ref[rows : rows + SUBLANES, :rows] = ids.astype(jnp.bfloat16)


def project_kernel(
    steps,
    counts_ref,
    x_ref,
    g_ref,
    a_ref,
    b_ref,
    of_ref,
    if_ref,
    rb_ref,
    ra_ref,
    out_ref,
    acc_x,
    acc_b,
    acc_o,
):
    step = pl.program_id(0)
    rank = a_ref.shape[0]
    rows = of_ref.shape[0]
    feat_size, copies, examples, part, _ = out_ref.shape
    seq = acc_x.shape[0] // examples

    @pl.when(step == 0)
    def _():
        acc_x[...] = jnp.zeros_like(acc_x)
        acc_b[...] = jnp.zeros_like(acc_b)
        acc_o[...] = jnp.zeros_like(acc_o)

    weights_x = jnp.concatenate([a_ref[...], if_ref[...]], axis=0)
    acc_x[...] += dot32(x_ref[...], weights_x, NT)
    acc_b[...] += dot32(g_ref[...], b_ref[...], NN)
    acc_o[...] += dot32(g_ref[...], of_ref[...], NT)

    @pl.when(step == steps - 1)
    def _():
        hidden = acc_x[:, :rank].astype(jnp.bfloat16)
        back = acc_b[...].astype(jnp.bfloat16)
        hidden_rank = dot32(hidden, rb_ref[...], NN).astype(jnp.bfloat16)
        back_rank = dot32(back, ra_ref[...], NN).astype(jnp.bfloat16)
        place = lax.broadcasted_iota(jnp.int32, (seq, rows), 0)
        for e in range(examples):
            span = slice(e * seq, (e + 1) * seq)
            live = place < counts_ref[e]
            gp = jnp.where(live, acc_o[span, :], 0.0).astype(jnp.bfloat16)
            ip = jnp.where(live, acc_x[span, rank:], 0.0).astype(jnp.bfloat16)
            term = dot32(gp, hidden_rank[span], TN) + dot32(ip, back_rank[span], TN)
            term = (term / counts_ref[e].astype(jnp.float32)).astype(jnp.bfloat16)
            for f in range(feat_size):
                for q in range(copies):
                    out_ref[f, q, e] = term[f * part : (f + 1) * part]


def project(counts, x, g, a, b, of_t, if_t, rb, ra, feat_size, copies, examples):
    tokens, width = x.shape
    rank = a.shape[0]
    rows = of_t.shape[0]
    cols = rb.shape[1]
    steps = 10
    kb = width // steps
    part = rows // feat_size
    whole = lambda shape: pl.BlockSpec(shape, lambda k: (0,) * len(shape))
    out = (feat_size, copies, examples, part, cols)
    return pl.pallas_call(
        functools.partial(project_kernel, steps),
        grid=(steps,),
        in_specs=[
            pl.BlockSpec(memory_space=pltpu.SMEM),
            pl.BlockSpec((tokens, kb), lambda k: (0, k)),
            pl.BlockSpec((tokens, kb), lambda k: (0, k)),
            pl.BlockSpec((rank, kb), lambda k: (0, k)),
            pl.BlockSpec((kb, rank), lambda k: (k, 0)),
            pl.BlockSpec((rows, kb), lambda k: (0, k)),
            pl.BlockSpec((rows, kb), lambda k: (0, k)),
            whole(rb.shape),
            whole(ra.shape),
        ],
        out_specs=whole(out),
        out_shape=jax.ShapeDtypeStruct(out, jnp.bfloat16),
        scratch_shapes=[
            pltpu.VMEM((tokens, rank + rows), jnp.float32),
            pltpu.VMEM((tokens, rank), jnp.float32),
            pltpu.VMEM((tokens, rows), jnp.float32),
        ],
        cost_estimate=pl.CostEstimate(
            flops=4 * tokens * width * (rank + rows),
            bytes_accessed=2 * (2 * tokens + 2 * rank + 2 * rows) * width,
            transcendentals=0,
        ),
        compiler_params=limit(16),
        name="project",
    )(counts, x, g, a, b, of_t, if_t, rb, ra)


def combine_kernel(rows, index_ref, parts_ref, *rest):
    pieces = rest[:-4]
    feat_ref, pack_ref, summed, flat = rest[-4:]
    feat_size, copies, examples, part, cols = parts_ref.shape
    width = part * cols
    members = copies * examples
    total = parts_ref[0].astype(jnp.float32)
    for f in range(1, feat_size):
        total = total + parts_ref[f].astype(jnp.float32)
    summed[...] = total.reshape(members * part, cols)
    flat[...] = jnp.zeros_like(flat)
    mine = index_ref[0] * (examples * part)
    for k in range(part):
        span = slice(k * cols, (k + 1) * cols)
        flat[:members, span] = summed[pl.ds(k, members, stride=part), :]
        feat_ref[:, span] = summed[pl.ds(mine + k, examples, stride=part), :].astype(jnp.bfloat16)
    features = flat[...].astype(jnp.bfloat16)
    rounded = features.astype(jnp.float32)
    norm = jnp.sum(rounded * rounded, axis=1, keepdims=True)
    count = len(pieces) * rows
    vals = jnp.concatenate([ref[:rows, :] for ref in pieces], axis=0)
    inner = dot32(features, vals, NT)
    squares = jnp.zeros((count, LANES), jnp.float32)
    for c in range(0, width, LANES):
        piece = vals[:, c : c + LANES].astype(jnp.float32)
        squares = squares + piece * piece
    val_norm = dot32(jnp.ones((SUBLANES, LANES), jnp.float32), squares, NT, HIGHEST)
    ids = jnp.concatenate(
        [ref[rows : rows + SUBLANES, :rows].astype(jnp.float32) for ref in pieces], axis=1
    )
    pack_ref[...] = jnp.full(pack_ref.shape, -1.0, jnp.float32)
    lanes = pack_ref.shape[-1]
    for q in range(copies):
        span = slice(q * examples, (q + 1) * examples)
        wide = jnp.broadcast_to(norm[span], (examples, lanes))
        for f in range(feat_size):
            pack_ref[f, q, :examples, :count] = inner[span]
            pack_ref[f, q, examples : 2 * examples, :] = wide
            pack_ref[f, q, 2 * examples : 2 * examples + 1, :count] = val_norm[:1]
            pack_ref[f, q, 2 * examples + 1 : 2 * examples + 2, :count] = ids[:1]


def score_kernel(count, scale, packs_ref, out_ref):
    feat_size, copies, _, lanes = packs_ref.shape
    examples = out_ref.shape[0]
    total = packs_ref[0]
    for f in range(1, feat_size):
        total = total + packs_ref[f]
    inner = total[:, :examples, :count]
    norm = total[0, examples : 2 * examples, :count]
    val_norm = total[:, 2 * examples : 2 * examples + 1, :count]
    ids = packs_ref[0, :, 2 * examples + 1 : 2 * examples + 2, :count]
    root = lax.rsqrt(norm + norm_eps)
    sums = jnp.zeros((examples, DOMAINS), jnp.float32)
    sizes = jnp.zeros((examples, DOMAINS), jnp.float32)
    ones = jnp.ones((examples, count), jnp.float32)
    domain = lax.broadcasted_iota(jnp.int32, (DOMAINS, count), 0).astype(jnp.float32)
    for q in range(copies):
        cosine = inner[q] * root * lax.rsqrt(val_norm[q] + norm_eps)
        marks = jnp.where(jnp.broadcast_to(ids[q], domain.shape) == domain, 1.0, 0.0)
        sums = sums + dot32(cosine, marks, NT, HIGHEST)
        sizes = sizes + dot32(ones, marks, NT)
    out_ref[...] = scale * sums / sizes


def axis_count(sizes, names):
    total = 1
    for name in names:
        total *= sizes[name]
    return total


def local(
    sizes,
    layer_inputs,
    output_grads,
    adapter_a,
    adapter_b,
    out_factor,
    in_factor,
    rank_factor_b,
    rank_factor_a,
    token_counts,
    val_grads,
    val_domain,
):
    _, examples, seq_len, width = layer_inputs.shape
    val_rows, val_cols = val_grads.shape
    feat_size = sizes["feat"]
    copies = axis_count(sizes, NEAR)
    far_size = axis_count(sizes, FAR)

    payload = pl.pallas_call(
        payload_kernel,
        out_shape=jax.ShapeDtypeStruct((val_rows + SUBLANES, val_cols), jnp.bfloat16),
        compiler_params=limit(4),
        name="payload",
    )(val_grads, val_domain.T)
    pieces = [payload]
    for s in range(1, far_size):
        pairs = [(i, (i + s) % far_size) for i in range(far_size)]
        pieces.append(lax.ppermute(payload, FAR, pairs))

    parts = project(
        token_counts,
        layer_inputs.reshape(examples * seq_len, width),
        output_grads.reshape(examples * seq_len, width),
        adapter_a[0],
        adapter_b[0],
        out_factor[0].T,
        in_factor[0].T,
        rank_factor_b[0],
        rank_factor_a[0],
        feat_size,
        copies,
        examples,
    )
    group = ("feat",) + NEAR
    members = feat_size * copies
    flat_parts = parts.reshape((members,) + parts.shape[2:])
    got = lax.all_to_all(flat_parts, group, 0, 0, tiled=True).reshape(parts.shape)

    count = far_size * val_rows
    lanes = round_up(count, LANES)
    block_rows = round_up(2 * examples + 2, SUBLANES)
    part, cols = parts.shape[3:]
    index = lax.axis_index(NEAR).astype(jnp.int32).reshape(1)
    smem = pl.BlockSpec(memory_space=pltpu.SMEM)
    vmem = pl.BlockSpec(memory_space=pltpu.VMEM)
    train_features, packs = pl.pallas_call(
        functools.partial(combine_kernel, val_rows),
        in_specs=[smem] + [vmem] * (1 + far_size),
        out_shape=[
            jax.ShapeDtypeStruct((examples, val_cols), jnp.bfloat16),
            jax.ShapeDtypeStruct((feat_size, copies, block_rows, lanes), jnp.float32),
        ],
        scratch_shapes=[
            pltpu.VMEM((copies * examples * part, cols), jnp.float32),
            pltpu.VMEM((round_up(copies * examples, 2 * SUBLANES), val_cols), jnp.float32),
        ],
        compiler_params=limit(8),
        name="combine",
    )(index, got, *pieces)

    flat_packs = packs.reshape((members,) + packs.shape[2:])
    returned = lax.all_to_all(flat_packs, group, 0, 0, tiled=True).reshape(packs.shape)
    domain_scores = pl.pallas_call(
        functools.partial(score_kernel, count, math.sqrt(PROJ)),
        out_shape=jax.ShapeDtypeStruct((examples, DOMAINS), jnp.float32),
        compiler_params=limit(4),
        name="score",
    )(returned)
    return (train_features, domain_scores)


def solution(mesh):
    in_specs = (
        P("feat", DP, None, None),
        P("feat", DP, None, None),
        P("feat", None, None),
        P("feat", None, None),
        P("feat", None, None),
        P("feat", None, None),
        P("feat", None, None),
        P("feat", None, None),
        P(DP),
        P(DP, "feat"),
        P(DP, None),
    )
    out_specs = (P(DP, "feat"), P(DP, None))
    feat_size, dp_size = mesh.shape["feat"], mesh.shape["dp"]
    sizes = {"feat": feat_size, "hi": dp_size // 4, "lo": 2, "core": 2}
    split = Mesh(mesh.devices.reshape(tuple(sizes.values())), tuple(sizes))
    body = functools.partial(local, sizes)
    return jax.shard_map(body, mesh=split, in_specs=in_specs, out_specs=out_specs, check_vma=False)
```

```python
import functools
import math

import jax
import jax.numpy as jnp
from jax import lax
from jax.experimental import pallas as pl
from jax.experimental.pallas import tpu as pltpu
from jax.sharding import Mesh
from jax.sharding import PartitionSpec as P

PROJ = 8192
DOMAINS = 8
LANES = 128
SUBLANES = 8
CHUNKS = 4
PROJECT_VMEM = 67_043_328 - 614_400

FAR = ("hi",)
NEAR = ("lo", "core")
DP = ("hi", "lo", "core")

norm_eps = 1e-06

NT = (((1,), (1,)), ((), ()))
NN = (((1,), (0,)), ((), ()))
TN = (((0,), (0,)), ((), ()))
HIGHEST = lax.Precision.HIGHEST


def dot32(left, right, dims, precision=None):
    return lax.dot_general(
        left, right, dims, precision=precision, preferred_element_type=jnp.float32
    )


def limit(mib):
    return pltpu.CompilerParams(vmem_limit_bytes=mib << 20)


def round_up(value, unit):
    return (value + unit - 1) // unit * unit


def project_kernel(
    counts_ref,
    x_hbm,
    g_hbm,
    a_hbm,
    b_hbm,
    of_hbm,
    if_hbm,
    rb_hbm,
    ra_hbm,
    out_ref,
    x_ref,
    g_ref,
    wx_ref,
    b_ref,
    of_ref,
    rb_ref,
    ra_ref,
    acc_x,
    acc_g,
    x_sems,
    g_sems,
    sems,
):
    feat_size, copies, examples, part, _ = out_ref.shape
    chunks, tokens, chunk = x_ref.shape
    seq = tokens // examples
    rank = a_hbm.shape[0]
    rows = of_hbm.shape[0]

    def x_moves(c):
        span = pl.ds(pl.multiple_of(c * chunk, LANES), chunk)
        return (
            pltpu.make_async_copy(x_hbm.at[:, span], x_ref.at[c], x_sems.at[c, 0]),
            pltpu.make_async_copy(a_hbm.at[:, span], wx_ref.at[c, :rank], x_sems.at[c, 1]),
            pltpu.make_async_copy(if_hbm.at[:, span], wx_ref.at[c, rank:], x_sems.at[c, 2]),
        )

    def g_moves(c):
        span = pl.ds(pl.multiple_of(c * chunk, LANES), chunk)
        return (
            pltpu.make_async_copy(g_hbm.at[:, span], g_ref.at[c], g_sems.at[c, 0]),
            pltpu.make_async_copy(b_hbm.at[span, :], b_ref.at[c], g_sems.at[c, 1]),
            pltpu.make_async_copy(of_hbm.at[:, span], of_ref.at[c], g_sems.at[c, 2]),
        )

    small = [
        pltpu.make_async_copy(rb_hbm, rb_ref, sems.at[0]),
        pltpu.make_async_copy(ra_hbm, ra_ref, sems.at[1]),
    ]

    @pl.loop(0, chunks)
    def _(c):
        for move in x_moves(c):
            move.start()

    for move in small:
        move.start()

    @pl.loop(0, chunks)
    def _(c):
        for move in g_moves(c):
            move.start()

    acc_x[...] = jnp.zeros_like(acc_x)
    acc_g[...] = jnp.zeros_like(acc_g)

    @pl.loop(0, chunks)
    def _(c):
        for move in x_moves(c):
            move.wait()
        acc_x[...] += dot32(x_ref[c], wx_ref[c], NT)

    for move in small:
        move.wait()

    @pl.loop(0, chunks)
    def _(c):
        for move in g_moves(c):
            move.wait()
        weights = jnp.concatenate([b_ref[c], of_ref[c].T], axis=1)
        acc_g[...] += dot32(g_ref[c], weights, NN)

    place = lax.broadcasted_iota(jnp.int32, (seq, rows), 0)

    @pl.loop(0, examples)
    def _(e):
        span = pl.ds(pl.multiple_of(e * seq, seq), seq)
        live = place < counts_ref[e]
        hidden = acc_x[span, :rank].astype(jnp.bfloat16)
        back = acc_g[span, :rank].astype(jnp.bfloat16)
        hidden_rank = dot32(hidden, rb_ref[...], NN).astype(jnp.bfloat16)
        back_rank = dot32(back, ra_ref[...], NN).astype(jnp.bfloat16)
        gp = jnp.where(live, acc_g[span, rank:], 0.0).astype(jnp.bfloat16)
        ip = jnp.where(live, acc_x[span, rank:], 0.0).astype(jnp.bfloat16)
        term = dot32(gp, hidden_rank, TN) + dot32(ip, back_rank, TN)
        term = (term / counts_ref[e].astype(jnp.float32)).astype(jnp.bfloat16)
        for f in range(feat_size):
            for q in range(copies):
                out_ref[f, q, e] = term[f * part : (f + 1) * part]


def project(counts, arrays, feat_size, copies, examples):
    x, _, a, _, of_t, _, rb, _ = arrays
    tokens, width = x.shape
    rank, rows = a.shape[0], of_t.shape[0]
    chunk = width // CHUNKS
    out = (feat_size, copies, examples, rows // feat_size, rb.shape[1])
    hbm = pl.BlockSpec(memory_space=pltpu.HBM)
    vmem = pl.BlockSpec(memory_space=pltpu.VMEM)
    low = [
        (CHUNKS, tokens, chunk),
        (CHUNKS, tokens, chunk),
        (CHUNKS, rank + rows, chunk),
        (CHUNKS, chunk, rank),
        (CHUNKS, rows, chunk),
        rb.shape,
        rb.shape,
    ]
    return pl.pallas_call(
        project_kernel,
        in_specs=[pl.BlockSpec(memory_space=pltpu.SMEM)] + [hbm] * len(arrays),
        out_specs=vmem,
        out_shape=jax.ShapeDtypeStruct(out, jnp.bfloat16),
        scratch_shapes=[pltpu.VMEM(shape, jnp.bfloat16) for shape in low]
        + [
            pltpu.VMEM((tokens, rank + rows), jnp.float32),
            pltpu.VMEM((tokens, rank + rows), jnp.float32),
            pltpu.SemaphoreType.DMA((CHUNKS, 3)),
            pltpu.SemaphoreType.DMA((CHUNKS, 3)),
            pltpu.SemaphoreType.DMA((2,)),
        ],
        cost_estimate=pl.CostEstimate(
            flops=4 * tokens * width * (rank + rows),
            bytes_accessed=2 * (2 * tokens + 2 * rank + 2 * rows) * width,
            transcendentals=0,
        ),
        compiler_params=pltpu.CompilerParams(vmem_limit_bytes=PROJECT_VMEM),
        name="project",
    )(counts, *arrays)


def combine_kernel(index_ref, parts_ref, *rest):
    pieces = rest[: (len(rest) - 4) // 2]
    domains = rest[len(pieces) : -4]
    feat_ref, pack_ref, summed, flat = rest[-4:]
    feat_size, copies, examples, part, cols = parts_ref.shape
    width = part * cols
    members = copies * examples
    total = parts_ref[0].astype(jnp.float32)
    for f in range(1, feat_size):
        total = total + parts_ref[f].astype(jnp.float32)
    summed[...] = total.reshape(members * part, cols)
    flat[...] = jnp.zeros_like(flat)
    mine = index_ref[0] * (examples * part)
    for k in range(part):
        span = slice(k * cols, (k + 1) * cols)
        flat[:members, span] = summed[pl.ds(k, members, stride=part), :]
        feat_ref[:, span] = summed[pl.ds(mine + k, examples, stride=part), :].astype(jnp.bfloat16)
    features = flat[...].astype(jnp.bfloat16)
    rounded = features.astype(jnp.float32)
    norm = jnp.sum(rounded * rounded, axis=1, keepdims=True)
    vals = jnp.concatenate([ref[...] for ref in pieces], axis=0)
    count = vals.shape[0]
    inner = dot32(features, vals, NT)
    squares = jnp.zeros((count, LANES), jnp.float32)
    for c in range(0, width, LANES):
        piece = vals[:, c : c + LANES].astype(jnp.float32)
        squares = squares + piece * piece
    val_norm = dot32(jnp.ones((SUBLANES, LANES), jnp.float32), squares, NT, HIGHEST)
    ids = jnp.concatenate([ref[...].astype(jnp.float32) for ref in domains], axis=1)
    pack_ref[...] = jnp.full(pack_ref.shape, -1.0, jnp.float32)
    lanes = pack_ref.shape[-1]
    for q in range(copies):
        span = slice(q * examples, (q + 1) * examples)
        wide = jnp.broadcast_to(norm[span], (examples, lanes))
        for f in range(feat_size):
            pack_ref[f, q, :examples, :count] = inner[span]
            pack_ref[f, q, examples : 2 * examples, :] = wide
            pack_ref[f, q, 2 * examples : 2 * examples + 1, :count] = val_norm[:1]
            pack_ref[f, q, 2 * examples + 1 : 2 * examples + 2, :count] = ids[:1]


def score_kernel(count, scale, packs_ref, out_ref):
    feat_size, copies, _, _ = packs_ref.shape
    examples = out_ref.shape[0]
    total = packs_ref[0]
    for f in range(1, feat_size):
        total = total + packs_ref[f]
    inner = total[:, :examples, :count]
    norm = total[0, examples : 2 * examples, :count]
    val_norm = total[:, 2 * examples : 2 * examples + 1, :count]
    ids = packs_ref[0, :, 2 * examples + 1 : 2 * examples + 2, :count]
    root = lax.rsqrt(norm + norm_eps)
    sums = jnp.zeros((examples, DOMAINS), jnp.float32)
    sizes = jnp.zeros((examples, DOMAINS), jnp.float32)
    ones = jnp.ones((examples, count), jnp.float32)
    domain = lax.broadcasted_iota(jnp.int32, (DOMAINS, count), 0).astype(jnp.float32)
    for q in range(copies):
        cosine = inner[q] * root * lax.rsqrt(val_norm[q] + norm_eps)
        marks = jnp.where(jnp.broadcast_to(ids[q], domain.shape) == domain, 1.0, 0.0)
        sums = sums + dot32(cosine, marks, NT, HIGHEST)
        sizes = sizes + dot32(ones, marks, NT)
    out_ref[...] = scale * sums / sizes


def axis_count(sizes, names):
    total = 1
    for name in names:
        total *= sizes[name]
    return total


def local(
    sizes,
    layer_inputs,
    output_grads,
    adapter_a,
    adapter_b,
    out_factor,
    in_factor,
    rank_factor_b,
    rank_factor_a,
    token_counts,
    val_grads,
    val_domain,
):
    _, examples, seq_len, width = layer_inputs.shape
    val_rows, val_cols = val_grads.shape
    feat_size = sizes["feat"]
    copies = axis_count(sizes, NEAR)
    far_size = axis_count(sizes, FAR)

    vals, domains = [val_grads], [val_domain.T]
    for s in range(1, far_size):
        pairs = [(i, (i + s) % far_size) for i in range(far_size)]
        vals.append(lax.ppermute(vals[0], FAR, pairs))
        domains.append(lax.ppermute(domains[0], FAR, pairs))

    arrays = (
        layer_inputs.reshape(examples * seq_len, width),
        output_grads.reshape(examples * seq_len, width),
        adapter_a[0],
        adapter_b[0],
        out_factor[0].T,
        in_factor[0].T,
        rank_factor_b[0],
        rank_factor_a[0],
    )
    parts = project(token_counts, arrays, feat_size, copies, examples)
    group = ("feat",) + NEAR
    members = feat_size * copies
    flat_parts = parts.reshape((members,) + parts.shape[2:])
    got = lax.all_to_all(flat_parts, group, 0, 0, tiled=True).reshape(parts.shape)

    count = far_size * val_rows
    lanes = round_up(count, LANES)
    block_rows = round_up(2 * examples + 2, SUBLANES)
    part, cols = parts.shape[3:]
    index = lax.axis_index(NEAR).astype(jnp.int32).reshape(1)
    smem = pl.BlockSpec(memory_space=pltpu.SMEM)
    vmem = pl.BlockSpec(memory_space=pltpu.VMEM)
    train_features, packs = pl.pallas_call(
        combine_kernel,
        in_specs=[smem] + [vmem] * (1 + 2 * far_size),
        out_shape=[
            jax.ShapeDtypeStruct((examples, val_cols), jnp.bfloat16),
            jax.ShapeDtypeStruct((feat_size, copies, block_rows, lanes), jnp.float32),
        ],
        scratch_shapes=[
            pltpu.VMEM((copies * examples * part, cols), jnp.float32),
            pltpu.VMEM((round_up(copies * examples, 2 * SUBLANES), val_cols), jnp.float32),
        ],
        compiler_params=limit(8),
        name="combine",
    )(index, got, *vals, *domains)

    flat_packs = packs.reshape((members,) + packs.shape[2:])
    returned = lax.all_to_all(flat_packs, group, 0, 0, tiled=True).reshape(packs.shape)
    domain_scores = pl.pallas_call(
        functools.partial(score_kernel, count, math.sqrt(PROJ)),
        out_shape=jax.ShapeDtypeStruct((examples, DOMAINS), jnp.float32),
        compiler_params=limit(4),
        name="score",
    )(returned)
    return (train_features, domain_scores)


def solution(mesh):
    in_specs = (
        P("feat", DP, None, None),
        P("feat", DP, None, None),
        P("feat", None, None),
        P("feat", None, None),
        P("feat", None, None),
        P("feat", None, None),
        P("feat", None, None),
        P("feat", None, None),
        P(DP),
        P(DP, "feat"),
        P(DP, None),
    )
    out_specs = (P(DP, "feat"), P(DP, None))
    feat_size, dp_size = mesh.shape["feat"], mesh.shape["dp"]
    sizes = {"feat": feat_size, "hi": dp_size // 4, "lo": 2, "core": 2}
    split = Mesh(mesh.devices.reshape(tuple(sizes.values())), tuple(sizes))
    body = functools.partial(local, sizes)
    return jax.shard_map(body, mesh=split, in_specs=in_specs, out_specs=out_specs, check_vma=False)
```

```python
import functools
import math

import jax
import jax.numpy as jnp
from jax import lax
from jax.experimental import pallas as pl
from jax.experimental.pallas import tpu as pltpu
from jax.sharding import Mesh
from jax.sharding import PartitionSpec as P

PROJ = 8192
DOMAINS = 8
LANES = 128
SUBLANES = 8
CHUNKS = 4
PROJECT_VMEM = 67_043_328 - 1_300_000

FAR = ("hi", "lo")
NEAR = ("core",)
DP = ("hi", "lo", "core")

norm_eps = 1e-06


NT = (((1,), (1,)), ((), ()))
NN = (((1,), (0,)), ((), ()))
TN = (((0,), (0,)), ((), ()))
HIGHEST = lax.Precision.HIGHEST


def dot32(left, right, dims, precision=None):
    return lax.dot_general(
        left, right, dims, precision=precision, preferred_element_type=jnp.float32
    )


def limit(mib):
    return pltpu.CompilerParams(vmem_limit_bytes=mib << 20)


def round_up(value, unit):
    return (value + unit - 1) // unit * unit


def payload_kernel(val_hbm, domain_hbm, out_ref, domain_ref, sems):
    rows = val_hbm.shape[0]
    moves = [
        pltpu.make_async_copy(domain_hbm, domain_ref, sems.at[0]),
        pltpu.make_async_copy(val_hbm, out_ref.at[:rows, :], sems.at[1]),
    ]
    for move in moves:
        move.start()
    out_ref[rows:, :] = jnp.zeros_like(out_ref[rows:, :])
    moves[0].wait()
    ids = jnp.broadcast_to(domain_ref[...].astype(jnp.float32), (SUBLANES, rows))
    out_ref[rows:, :rows] = ids.astype(jnp.bfloat16)
    moves[1].wait()


def project_kernel(
    counts_ref,
    x_hbm,
    g_hbm,
    a_hbm,
    b_hbm,
    of_hbm,
    if_hbm,
    rb_hbm,
    ra_hbm,
    out_ref,
    x_ref,
    g_ref,
    wx_ref,
    b_ref,
    of_ref,
    rb_ref,
    ra_ref,
    acc_x,
    acc_g,
    x_sems,
    g_sems,
    sems,
):
    feat_size, copies, examples, part, _ = out_ref.shape
    chunks, tokens, chunk = x_ref.shape
    seq = tokens // examples
    rank = a_hbm.shape[0]
    rows = of_hbm.shape[0]

    def x_moves(c):
        span = pl.ds(pl.multiple_of(c * chunk, LANES), chunk)
        return (
            pltpu.make_async_copy(x_hbm.at[:, span], x_ref.at[c], x_sems.at[c, 0]),
            pltpu.make_async_copy(a_hbm.at[:, span], wx_ref.at[c, :rank], x_sems.at[c, 1]),
            pltpu.make_async_copy(if_hbm.at[:, span], wx_ref.at[c, rank:], x_sems.at[c, 2]),
        )

    def g_moves(c):
        span = pl.ds(pl.multiple_of(c * chunk, LANES), chunk)
        return (
            pltpu.make_async_copy(g_hbm.at[:, span], g_ref.at[c], g_sems.at[c, 0]),
            pltpu.make_async_copy(b_hbm.at[span, :], b_ref.at[c], g_sems.at[c, 1]),
            pltpu.make_async_copy(of_hbm.at[:, span], of_ref.at[c], g_sems.at[c, 2]),
        )

    small = [
        pltpu.make_async_copy(rb_hbm, rb_ref, sems.at[0]),
        pltpu.make_async_copy(ra_hbm, ra_ref, sems.at[1]),
    ]

    @pl.loop(0, chunks)
    def _(c):
        for move in x_moves(c):
            move.start()

    for move in small:
        move.start()

    @pl.loop(0, chunks)
    def _(c):
        for move in g_moves(c):
            move.start()

    acc_x[...] = jnp.zeros_like(acc_x)
    acc_g[...] = jnp.zeros_like(acc_g)

    @pl.loop(0, chunks)
    def _(c):
        for move in x_moves(c):
            move.wait()
        acc_x[...] += dot32(x_ref[c], wx_ref[c], NT)

    for move in small:
        move.wait()

    @pl.loop(0, chunks)
    def _(c):
        for move in g_moves(c):
            move.wait()
        weights = jnp.concatenate([b_ref[c], of_ref[c].T], axis=1)
        acc_g[...] += dot32(g_ref[c], weights, NN)

    place = lax.broadcasted_iota(jnp.int32, (seq, rows), 0)

    @pl.loop(0, examples)
    def _(e):
        span = pl.ds(pl.multiple_of(e * seq, seq), seq)
        live = place < counts_ref[e]
        hidden = acc_x[span, :rank].astype(jnp.bfloat16)
        back = acc_g[span, :rank].astype(jnp.bfloat16)
        hidden_rank = dot32(hidden, rb_ref[...], NN).astype(jnp.bfloat16)
        back_rank = dot32(back, ra_ref[...], NN).astype(jnp.bfloat16)
        gp = jnp.where(live, acc_g[span, rank:], 0.0).astype(jnp.bfloat16)
        ip = jnp.where(live, acc_x[span, rank:], 0.0).astype(jnp.bfloat16)
        term = dot32(gp, hidden_rank, TN) + dot32(ip, back_rank, TN)
        term = (term / counts_ref[e].astype(jnp.float32)).astype(jnp.bfloat16)
        for f in range(feat_size):
            for q in range(copies):
                out_ref[f, q, e] = term[f * part : (f + 1) * part]


def project(counts, arrays, feat_size, copies, examples):
    x, _, a, _, of_t, _, rb, _ = arrays
    tokens, width = x.shape
    rank, rows = a.shape[0], of_t.shape[0]
    chunk = width // CHUNKS
    out = (feat_size, copies, examples, rows // feat_size, rb.shape[1])
    hbm = pl.BlockSpec(memory_space=pltpu.HBM)
    vmem = pl.BlockSpec(memory_space=pltpu.VMEM)
    low = [
        (CHUNKS, tokens, chunk),
        (CHUNKS, tokens, chunk),
        (CHUNKS, rank + rows, chunk),
        (CHUNKS, chunk, rank),
        (CHUNKS, rows, chunk),
        rb.shape,
        rb.shape,
    ]
    return pl.pallas_call(
        project_kernel,
        in_specs=[pl.BlockSpec(memory_space=pltpu.SMEM)] + [hbm] * len(arrays),
        out_specs=vmem,
        out_shape=pltpu.VMEM(out, jnp.bfloat16),
        scratch_shapes=[pltpu.VMEM(shape, jnp.bfloat16) for shape in low]
        + [
            pltpu.VMEM((tokens, rank + rows), jnp.float32),
            pltpu.VMEM((tokens, rank + rows), jnp.float32),
            pltpu.SemaphoreType.DMA((CHUNKS, 3)),
            pltpu.SemaphoreType.DMA((CHUNKS, 3)),
            pltpu.SemaphoreType.DMA((2,)),
        ],
        cost_estimate=pl.CostEstimate(
            flops=4 * tokens * width * (rank + rows),
            bytes_accessed=2 * (2 * tokens + 2 * rank + 2 * rows) * width,
            transcendentals=0,
        ),
        compiler_params=pltpu.CompilerParams(vmem_limit_bytes=PROJECT_VMEM),
        name="project",
    )(counts, *arrays)


def combine_kernel(rows, index_ref, parts_ref, *rest):
    pieces = rest[:-4]
    feat_ref, pack_ref, summed, flat = rest[-4:]
    feat_size, copies, examples, part, cols = parts_ref.shape
    width = part * cols
    members = copies * examples
    total = parts_ref[0].astype(jnp.float32)
    for f in range(1, feat_size):
        total = total + parts_ref[f].astype(jnp.float32)
    summed[...] = total.reshape(members * part, cols)
    flat[...] = jnp.zeros_like(flat)
    mine = index_ref[0] * (examples * part)
    for k in range(part):
        span = slice(k * cols, (k + 1) * cols)
        flat[:members, span] = summed[pl.ds(k, members, stride=part), :]
        feat_ref[:, span] = summed[pl.ds(mine + k, examples, stride=part), :].astype(jnp.bfloat16)
    features = flat[...].astype(jnp.bfloat16)
    rounded = features.astype(jnp.float32)
    norm = jnp.sum(rounded * rounded, axis=1, keepdims=True)
    vals = jnp.concatenate([ref[:rows, :] for ref in pieces], axis=0)
    count = vals.shape[0]
    inner = dot32(features, vals, NT)
    squares = jnp.zeros((count, LANES), jnp.float32)
    for c in range(0, width, LANES):
        piece = vals[:, c : c + LANES].astype(jnp.float32)
        squares = squares + piece * piece
    val_norm = dot32(jnp.ones((SUBLANES, LANES), jnp.float32), squares, NT, HIGHEST)
    ids = jnp.concatenate(
        [ref[rows : rows + SUBLANES, :rows].astype(jnp.float32) for ref in pieces], axis=1
    )
    pack_ref[...] = jnp.full(pack_ref.shape, -1.0, jnp.float32)
    lanes = pack_ref.shape[-1]
    for q in range(copies):
        span = slice(q * examples, (q + 1) * examples)
        wide = jnp.broadcast_to(norm[span], (examples, lanes))
        for f in range(feat_size):
            pack_ref[f, q, :examples, :count] = inner[span]
            pack_ref[f, q, examples : 2 * examples, :] = wide
            pack_ref[f, q, 2 * examples : 2 * examples + 1, :count] = val_norm[:1]
            pack_ref[f, q, 2 * examples + 1 : 2 * examples + 2, :count] = ids[:1]


def score_kernel(count, scale, packs_ref, out_ref):
    feat_size, copies, _, _ = packs_ref.shape
    examples = out_ref.shape[0]
    total = packs_ref[0]
    for f in range(1, feat_size):
        total = total + packs_ref[f]
    inner = total[:, :examples, :count]
    norm = total[0, examples : 2 * examples, :count]
    val_norm = total[:, 2 * examples : 2 * examples + 1, :count]
    ids = packs_ref[0, :, 2 * examples + 1 : 2 * examples + 2, :count]
    root = lax.rsqrt(norm + norm_eps)
    sums = jnp.zeros((examples, DOMAINS), jnp.float32)
    sizes = jnp.zeros((examples, DOMAINS), jnp.float32)
    ones = jnp.ones((examples, count), jnp.float32)
    domain = lax.broadcasted_iota(jnp.int32, (DOMAINS, count), 0).astype(jnp.float32)
    for q in range(copies):
        cosine = inner[q] * root * lax.rsqrt(val_norm[q] + norm_eps)
        marks = jnp.where(jnp.broadcast_to(ids[q], domain.shape) == domain, 1.0, 0.0)
        sums = sums + dot32(cosine, marks, NT, HIGHEST)
        sizes = sizes + dot32(ones, marks, NT)
    out_ref[...] = scale * sums / sizes


def axis_count(sizes, names):
    total = 1
    for name in names:
        total *= sizes[name]
    return total


def local(
    sizes,
    layer_inputs,
    output_grads,
    adapter_a,
    adapter_b,
    out_factor,
    in_factor,
    rank_factor_b,
    rank_factor_a,
    token_counts,
    val_grads,
    val_domain,
):
    _, examples, seq_len, width = layer_inputs.shape
    val_rows, val_cols = val_grads.shape
    feat_size = sizes["feat"]
    copies = axis_count(sizes, NEAR)
    far_size = axis_count(sizes, FAR)

    payload = pl.pallas_call(
        payload_kernel,
        in_specs=[pl.BlockSpec(memory_space=pltpu.HBM)] * 2,
        out_specs=pl.BlockSpec(memory_space=pltpu.VMEM),
        out_shape=pltpu.VMEM((val_rows + SUBLANES, val_cols), jnp.bfloat16),
        scratch_shapes=[
            pltpu.VMEM((1, val_rows), jnp.int32),
            pltpu.SemaphoreType.DMA((2,)),
        ],
        compiler_params=pltpu.CompilerParams(vmem_limit_bytes=PROJECT_VMEM),
        name="payload",
    )(val_grads, val_domain.T)
    pieces = [payload]
    for s in range(1, far_size):
        pairs = [(i, (i + s) % far_size) for i in range(far_size)]
        pieces.append(lax.ppermute(payload, FAR, pairs))

    arrays = (
        layer_inputs.reshape(examples * seq_len, width),
        output_grads.reshape(examples * seq_len, width),
        adapter_a[0],
        adapter_b[0],
        out_factor[0].T,
        in_factor[0].T,
        rank_factor_b[0],
        rank_factor_a[0],
    )
    parts = project(token_counts, arrays, feat_size, copies, examples)
    group = ("feat",) + NEAR
    members = feat_size * copies
    index = lax.axis_index(NEAR).astype(jnp.int32).reshape(1)
    parts, index = lax.optimization_barrier((parts, index))
    flat_parts = parts.reshape((members,) + parts.shape[2:])
    got = lax.all_to_all(flat_parts, group, 0, 0, tiled=True).reshape(parts.shape)

    count = far_size * val_rows
    lanes = round_up(count, LANES)
    block_rows = round_up(2 * examples + 2, SUBLANES)
    part, cols = parts.shape[3:]
    smem = pl.BlockSpec(memory_space=pltpu.SMEM)
    vmem = pl.BlockSpec(memory_space=pltpu.VMEM)
    train_features, packs = pl.pallas_call(
        functools.partial(combine_kernel, val_rows),
        in_specs=[smem] + [vmem] * (1 + far_size),
        out_shape=[
            jax.ShapeDtypeStruct((examples, val_cols), jnp.bfloat16),
            jax.ShapeDtypeStruct((feat_size, copies, block_rows, lanes), jnp.float32),
        ],
        scratch_shapes=[
            pltpu.VMEM((copies * examples * part, cols), jnp.float32),
            pltpu.VMEM((round_up(copies * examples, 2 * SUBLANES), val_cols), jnp.float32),
        ],
        compiler_params=limit(8),
        name="combine",
    )(index, got, *pieces)

    flat_packs = packs.reshape((members,) + packs.shape[2:])
    returned = lax.all_to_all(flat_packs, group, 0, 0, tiled=True).reshape(packs.shape)
    domain_scores = pl.pallas_call(
        functools.partial(score_kernel, count, math.sqrt(PROJ)),
        out_shape=jax.ShapeDtypeStruct((examples, DOMAINS), jnp.float32),
        compiler_params=limit(4),
        name="score",
    )(returned)
    return (train_features, domain_scores)


def solution(mesh):
    in_specs = (
        P("feat", DP, None, None),
        P("feat", DP, None, None),
        P("feat", None, None),
        P("feat", None, None),
        P("feat", None, None),
        P("feat", None, None),
        P("feat", None, None),
        P("feat", None, None),
        P(DP),
        P(DP, "feat"),
        P(DP, None),
    )
    out_specs = (P(DP, "feat"), P(DP, None))
    feat_size, dp_size = mesh.shape["feat"], mesh.shape["dp"]
    sizes = {"feat": feat_size, "hi": dp_size // 4, "lo": 2, "core": 2}
    split = Mesh(mesh.devices.reshape(tuple(sizes.values())), tuple(sizes))
    body = functools.partial(local, sizes)
    return jax.shard_map(body, mesh=split, in_specs=in_specs, out_specs=out_specs, check_vma=False)
```

```python
import functools
import math

import jax
import jax.numpy as jnp
from jax import lax
from jax.experimental import pallas as pl
from jax.experimental.pallas import tpu as pltpu
from jax.sharding import Mesh
from jax.sharding import PartitionSpec as P

PROJ = 8192
DOMAINS = 8
LANES = 128
SUBLANES = 8
CHUNKS = 2
PROJECT_VMEM = 24 << 20

FAR = ("hi", "lo")
NEAR = ("core",)
DP = ("hi", "lo", "core")

norm_eps = 1e-06


NT = (((1,), (1,)), ((), ()))
NN = (((1,), (0,)), ((), ()))
TN = (((0,), (0,)), ((), ()))
HIGHEST = lax.Precision.HIGHEST


def dot32(left, right, dims, precision=None):
    return lax.dot_general(
        left, right, dims, precision=precision, preferred_element_type=jnp.float32
    )


def limit(mib):
    return pltpu.CompilerParams(vmem_limit_bytes=mib << 20)


def round_up(value, unit):
    return (value + unit - 1) // unit * unit


def payload_kernel(val_hbm, domain_hbm, out_ref, domain_ref, sems):
    rows = val_hbm.shape[0]
    moves = [
        pltpu.make_async_copy(domain_hbm, domain_ref, sems.at[0]),
        pltpu.make_async_copy(val_hbm, out_ref.at[:rows, :], sems.at[1]),
    ]
    for move in moves:
        move.start()
    out_ref[rows:, :] = jnp.zeros_like(out_ref[rows:, :])
    moves[0].wait()
    ids = jnp.broadcast_to(domain_ref[...].astype(jnp.float32), (SUBLANES, rows))
    out_ref[rows:, :rows] = ids.astype(jnp.bfloat16)
    moves[1].wait()


def project_kernel(
    counts_ref,
    x_hbm,
    g_hbm,
    a_ref,
    b_ref,
    of_hbm,
    if_hbm,
    rb_hbm,
    ra_hbm,
    out_ref,
    x_ref,
    g_ref,
    of_ref,
    if_ref,
    rb_ref,
    ra_ref,
    acc_x,
    acc_g,
    rank_ref,
    x_sems,
    g_sems,
    sems,
):
    feat_size, copies, examples, part, _ = out_ref.shape
    chunks, tokens, chunk = x_ref.shape
    seq = tokens // examples
    rank = a_ref.shape[0]
    rows = of_hbm.shape[0]

    def span_of(c):
        return pl.ds(pl.multiple_of(c * chunk, LANES), chunk)

    def x_moves(c):
        span = span_of(c)
        return (
            pltpu.make_async_copy(x_hbm.at[:, span], x_ref.at[c], x_sems.at[c, 0]),
            pltpu.make_async_copy(if_hbm.at[:, span], if_ref.at[c], x_sems.at[c, 1]),
        )

    def g_moves(c):
        span = span_of(c)
        return (
            pltpu.make_async_copy(g_hbm.at[:, span], g_ref.at[c], g_sems.at[c, 0]),
            pltpu.make_async_copy(of_hbm.at[:, span], of_ref.at[c], g_sems.at[c, 1]),
        )

    small = [
        pltpu.make_async_copy(rb_hbm, rb_ref, sems.at[0]),
        pltpu.make_async_copy(ra_hbm, ra_ref, sems.at[1]),
    ]

    @pl.loop(0, chunks)
    def _(c):
        for move in x_moves(c):
            move.start()

    for move in small:
        move.start()

    @pl.loop(0, chunks)
    def _(c):
        for move in g_moves(c):
            move.start()

    acc_x[...] = jnp.zeros_like(acc_x)
    acc_g[...] = jnp.zeros_like(acc_g)

    @pl.loop(0, chunks)
    def _(c):
        for move in x_moves(c):
            move.wait()
        weights = jnp.concatenate([a_ref[:, span_of(c)], if_ref[c]], axis=0)
        acc_x[...] += dot32(x_ref[c], weights, NT)

    for move in small:
        move.wait()
    place = lax.broadcasted_iota(jnp.int32, (seq, rows), 0)
    spans = [slice(e * seq, (e + 1) * seq) for e in range(examples)]
    live = [place < counts_ref[e] for e in range(examples)]
    hidden = acc_x[:, :rank].astype(jnp.bfloat16)
    rank_ref[...] = dot32(hidden, rb_ref[...], NN).astype(jnp.bfloat16)

    @pl.loop(0, chunks)
    def _(c):
        for move in g_moves(c):
            move.wait()
        weights = jnp.concatenate([b_ref[span_of(c), :], of_ref[c].T], axis=1)
        acc_g[...] += dot32(g_ref[c], weights, NN)

    back = acc_g[:, :rank].astype(jnp.bfloat16)
    back_rank = dot32(back, ra_ref[...], NN).astype(jnp.bfloat16)
    for e, span in enumerate(spans):
        gp = jnp.where(live[e], acc_g[span, rank:], 0.0).astype(jnp.bfloat16)
        ip = jnp.where(live[e], acc_x[span, rank:], 0.0).astype(jnp.bfloat16)
        term = dot32(gp, rank_ref[span, :], TN) + dot32(ip, back_rank[span], TN)
        term = (term / counts_ref[e].astype(jnp.float32)).astype(jnp.bfloat16)
        for f in range(feat_size):
            for q in range(copies):
                out_ref[f, q, e] = term[f * part : (f + 1) * part]


def project(counts, arrays, feat_size, copies, examples):
    x, _, a, _, of_t, _, rb, _ = arrays
    tokens, width = x.shape
    rank, rows = a.shape[0], of_t.shape[0]
    chunk = width // CHUNKS
    out = (feat_size, copies, examples, rows // feat_size, rb.shape[1])
    hbm = pl.BlockSpec(memory_space=pltpu.HBM)
    vmem = pl.BlockSpec(memory_space=pltpu.VMEM)
    fixed = [
        pltpu.with_memory_space_constraint(array, pltpu.HBM) if n not in (2, 3) else array
        for n, array in enumerate(arrays)
    ]
    low = [
        (CHUNKS, tokens, chunk),
        (CHUNKS, tokens, chunk),
        (CHUNKS, rows, chunk),
        (CHUNKS, rows, chunk),
        rb.shape,
        rb.shape,
    ]
    return pl.pallas_call(
        project_kernel,
        in_specs=[pl.BlockSpec(memory_space=pltpu.SMEM)] + [hbm] * 2 + [vmem] * 2 + [hbm] * 4,
        out_specs=vmem,
        out_shape=pltpu.VMEM(out, jnp.bfloat16),
        scratch_shapes=[pltpu.VMEM(shape, jnp.bfloat16) for shape in low]
        + [
            pltpu.VMEM((tokens, rank + rows), jnp.float32),
            pltpu.VMEM((tokens, rank + rows), jnp.float32),
            pltpu.VMEM((tokens, rb.shape[1]), jnp.bfloat16),
            pltpu.SemaphoreType.DMA((CHUNKS, 2)),
            pltpu.SemaphoreType.DMA((CHUNKS, 2)),
            pltpu.SemaphoreType.DMA((2,)),
        ],
        cost_estimate=pl.CostEstimate(
            flops=4 * tokens * width * (rank + rows),
            bytes_accessed=2 * (2 * tokens + 2 * rank + 2 * rows) * width,
            transcendentals=0,
        ),
        compiler_params=pltpu.CompilerParams(vmem_limit_bytes=PROJECT_VMEM),
        name="project",
    )(counts, *fixed)


def combine_kernel(rows, index_ref, parts_ref, *rest):
    pieces = rest[:-4]
    feat_ref, pack_ref, summed, flat = rest[-4:]
    feat_size, copies, examples, part, cols = parts_ref.shape
    width = part * cols
    members = copies * examples
    total = parts_ref[0].astype(jnp.float32)
    for f in range(1, feat_size):
        total = total + parts_ref[f].astype(jnp.float32)
    summed[...] = total.reshape(members * part, cols)
    flat[...] = jnp.zeros_like(flat)
    mine = index_ref[0] * (examples * part)
    for k in range(part):
        span = slice(k * cols, (k + 1) * cols)
        flat[:members, span] = summed[pl.ds(k, members, stride=part), :]
        feat_ref[:, span] = summed[pl.ds(mine + k, examples, stride=part), :].astype(jnp.bfloat16)
    features = flat[...].astype(jnp.bfloat16)
    rounded = features.astype(jnp.float32)
    norm = jnp.sum(rounded * rounded, axis=1, keepdims=True)
    vals = jnp.concatenate([ref[:rows, :] for ref in pieces], axis=0)
    count = vals.shape[0]
    inner = dot32(features, vals, NT)
    squares = jnp.zeros((count, LANES), jnp.float32)
    for c in range(0, width, LANES):
        piece = vals[:, c : c + LANES].astype(jnp.float32)
        squares = squares + piece * piece
    val_norm = dot32(jnp.ones((SUBLANES, LANES), jnp.float32), squares, NT, HIGHEST)
    ids = jnp.concatenate(
        [ref[rows : rows + SUBLANES, :rows].astype(jnp.float32) for ref in pieces], axis=1
    )
    pack_ref[...] = jnp.full(pack_ref.shape, -1.0, jnp.float32)
    lanes = pack_ref.shape[-1]
    for q in range(copies):
        span = slice(q * examples, (q + 1) * examples)
        wide = jnp.broadcast_to(norm[span], (examples, lanes))
        for f in range(feat_size):
            pack_ref[f, q, :examples, :count] = inner[span]
            pack_ref[f, q, examples : 2 * examples, :] = wide
            pack_ref[f, q, 2 * examples : 2 * examples + 1, :count] = val_norm[:1]
            pack_ref[f, q, 2 * examples + 1 : 2 * examples + 2, :count] = ids[:1]


def score_kernel(count, scale, packs_ref, out_ref):
    feat_size, copies, _, _ = packs_ref.shape
    examples = out_ref.shape[0]
    total = packs_ref[0]
    for f in range(1, feat_size):
        total = total + packs_ref[f]
    inner = total[:, :examples, :count]
    norm = total[0, examples : 2 * examples, :count]
    val_norm = total[:, 2 * examples : 2 * examples + 1, :count]
    ids = packs_ref[0, :, 2 * examples + 1 : 2 * examples + 2, :count]
    root = lax.rsqrt(norm + norm_eps)
    sums = jnp.zeros((examples, DOMAINS), jnp.float32)
    sizes = jnp.zeros((examples, DOMAINS), jnp.float32)
    ones = jnp.ones((examples, count), jnp.float32)
    domain = lax.broadcasted_iota(jnp.int32, (DOMAINS, count), 0).astype(jnp.float32)
    for q in range(copies):
        cosine = inner[q] * root * lax.rsqrt(val_norm[q] + norm_eps)
        marks = jnp.where(jnp.broadcast_to(ids[q], domain.shape) == domain, 1.0, 0.0)
        sums = sums + dot32(cosine, marks, NT, HIGHEST)
        sizes = sizes + dot32(ones, marks, NT)
    out_ref[...] = scale * sums / sizes


def axis_count(sizes, names):
    total = 1
    for name in names:
        total *= sizes[name]
    return total


def local(
    sizes,
    layer_inputs,
    output_grads,
    adapter_a,
    adapter_b,
    out_factor,
    in_factor,
    rank_factor_b,
    rank_factor_a,
    token_counts,
    val_grads,
    val_domain,
):
    _, examples, seq_len, width = layer_inputs.shape
    val_rows, val_cols = val_grads.shape
    feat_size = sizes["feat"]
    copies = axis_count(sizes, NEAR)
    far_size = axis_count(sizes, FAR)

    payload = pl.pallas_call(
        payload_kernel,
        in_specs=[pl.BlockSpec(memory_space=pltpu.HBM)] * 2,
        out_specs=pl.BlockSpec(memory_space=pltpu.VMEM),
        out_shape=pltpu.VMEM((val_rows + SUBLANES, val_cols), jnp.bfloat16),
        scratch_shapes=[
            pltpu.VMEM((1, val_rows), jnp.int32),
            pltpu.SemaphoreType.DMA((2,)),
        ],
        cost_estimate=pl.CostEstimate(
            flops=8_000_000_000, bytes_accessed=16_000_000, transcendentals=0
        ),
        compiler_params=limit(4),
        name="payload",
    )(
        pltpu.with_memory_space_constraint(val_grads, pltpu.HBM),
        pltpu.with_memory_space_constraint(val_domain.T, pltpu.HBM),
    )
    pieces = [payload]
    for s in range(1, far_size):
        pairs = [(i, (i + s) % far_size) for i in range(far_size)]
        pieces.append(lax.ppermute(payload, FAR, pairs))

    arrays = (
        layer_inputs.reshape(examples * seq_len, width),
        output_grads.reshape(examples * seq_len, width),
        adapter_a[0],
        adapter_b[0],
        out_factor[0].T,
        in_factor[0].T,
        rank_factor_b[0],
        rank_factor_a[0],
    )
    parts = project(token_counts, arrays, feat_size, copies, examples)
    group = ("feat",) + NEAR
    members = feat_size * copies
    index = lax.axis_index(NEAR).astype(jnp.int32).reshape(1)
    parts, index = lax.optimization_barrier((parts, index))
    flat_parts = parts.reshape((members,) + parts.shape[2:])
    got = lax.all_to_all(flat_parts, group, 0, 0, tiled=True).reshape(parts.shape)

    count = far_size * val_rows
    lanes = round_up(count, LANES)
    block_rows = round_up(2 * examples + 2, SUBLANES)
    part, cols = parts.shape[3:]
    smem = pl.BlockSpec(memory_space=pltpu.SMEM)
    vmem = pl.BlockSpec(memory_space=pltpu.VMEM)
    train_features, packs = pl.pallas_call(
        functools.partial(combine_kernel, val_rows),
        in_specs=[smem] + [vmem] * (1 + far_size),
        out_shape=[
            jax.ShapeDtypeStruct((examples, val_cols), jnp.bfloat16),
            jax.ShapeDtypeStruct((feat_size, copies, block_rows, lanes), jnp.float32),
        ],
        scratch_shapes=[
            pltpu.VMEM((copies * examples * part, cols), jnp.float32),
            pltpu.VMEM((round_up(copies * examples, 2 * SUBLANES), val_cols), jnp.float32),
        ],
        compiler_params=limit(8),
        name="combine",
    )(index, got, *pieces)

    flat_packs = packs.reshape((members,) + packs.shape[2:])
    returned = lax.all_to_all(flat_packs, group, 0, 0, tiled=True).reshape(packs.shape)
    domain_scores = pl.pallas_call(
        functools.partial(score_kernel, count, math.sqrt(PROJ)),
        out_shape=jax.ShapeDtypeStruct((examples, DOMAINS), jnp.float32),
        compiler_params=limit(4),
        name="score",
    )(returned)
    return (train_features, domain_scores)


def solution(mesh):
    in_specs = (
        P("feat", DP, None, None),
        P("feat", DP, None, None),
        P("feat", None, None),
        P("feat", None, None),
        P("feat", None, None),
        P("feat", None, None),
        P("feat", None, None),
        P("feat", None, None),
        P(DP),
        P(DP, "feat"),
        P(DP, None),
    )
    out_specs = (P(DP, "feat"), P(DP, None))
    feat_size, dp_size = mesh.shape["feat"], mesh.shape["dp"]
    sizes = {"feat": feat_size, "hi": dp_size // 4, "lo": 2, "core": 2}
    split = Mesh(mesh.devices.reshape(tuple(sizes.values())), tuple(sizes))
    body = functools.partial(local, sizes)
    return jax.shard_map(body, mesh=split, in_specs=in_specs, out_specs=out_specs, check_vma=False)
```

```python
import functools
import math

import jax
import jax.numpy as jnp
from jax import lax
from jax.experimental import pallas as pl
from jax.experimental.pallas import tpu as pltpu
from jax.sharding import Mesh
from jax.sharding import PartitionSpec as P

PROJ = 8192
DOMAINS = 8
LANES = 128
SUBLANES = 8
CHUNKS = 2
PROJECT_VMEM = 24 << 20

FAR = ("hi", "lo")
NEAR = ("core",)
DP = ("hi", "lo", "core")

norm_eps = 1e-06


NT = (((1,), (1,)), ((), ()))
NN = (((1,), (0,)), ((), ()))
TN = (((0,), (0,)), ((), ()))
HIGHEST = lax.Precision.HIGHEST


def dot32(left, right, dims, precision=None):
    return lax.dot_general(
        left, right, dims, precision=precision, preferred_element_type=jnp.float32
    )


def limit(mib):
    return pltpu.CompilerParams(vmem_limit_bytes=mib << 20)


def round_up(value, unit):
    return (value + unit - 1) // unit * unit


def payload_kernel(val_hbm, domain_hbm, out_ref, domain_ref, sems):
    rows, width = val_hbm.shape
    moves = [
        pltpu.make_async_copy(domain_hbm, domain_ref, sems.at[0]),
        pltpu.make_async_copy(val_hbm, out_ref.at[:, :width], sems.at[1]),
    ]
    for move in moves:
        move.start()
    moves[0].wait()
    ids = jnp.broadcast_to(domain_ref[...].astype(jnp.float32), (rows, rows))
    out_ref[:, width : width + rows] = ids.astype(jnp.bfloat16)
    moves[1].wait()


def project_kernel(
    counts_ref,
    x_hbm,
    g_hbm,
    a_ref,
    b_ref,
    of_hbm,
    if_hbm,
    rb_hbm,
    ra_hbm,
    out_ref,
    x_ref,
    g_ref,
    of_ref,
    if_ref,
    rb_ref,
    ra_ref,
    acc_x,
    acc_g,
    rank_ref,
    x_sems,
    g_sems,
    sems,
):
    feat_size, copies, examples, part, _ = out_ref.shape
    chunks, tokens, chunk = x_ref.shape
    seq = tokens // examples
    rank = a_ref.shape[0]
    rows = of_hbm.shape[0]

    def span_of(c):
        return pl.ds(pl.multiple_of(c * chunk, LANES), chunk)

    def x_moves(c):
        span = span_of(c)
        return (
            pltpu.make_async_copy(x_hbm.at[:, span], x_ref.at[c], x_sems.at[c, 0]),
            pltpu.make_async_copy(if_hbm.at[:, span], if_ref.at[c], x_sems.at[c, 1]),
        )

    def g_moves(c):
        span = span_of(c)
        return (
            pltpu.make_async_copy(g_hbm.at[:, span], g_ref.at[c], g_sems.at[c, 0]),
            pltpu.make_async_copy(of_hbm.at[:, span], of_ref.at[c], g_sems.at[c, 1]),
        )

    small = [
        pltpu.make_async_copy(rb_hbm, rb_ref, sems.at[0]),
        pltpu.make_async_copy(ra_hbm, ra_ref, sems.at[1]),
    ]

    @pl.loop(0, chunks)
    def _(c):
        for move in x_moves(c):
            move.start()

    for move in small:
        move.start()

    @pl.loop(0, chunks)
    def _(c):
        for move in g_moves(c):
            move.start(priority=1)

    acc_x[...] = jnp.zeros_like(acc_x)
    acc_g[...] = jnp.zeros_like(acc_g)

    @pl.loop(0, chunks)
    def _(c):
        for move in x_moves(c):
            move.wait()
        weights = jnp.concatenate([a_ref[:, span_of(c)], if_ref[c]], axis=0)
        acc_x[...] += dot32(x_ref[c], weights, NT)

    for move in small:
        move.wait()
    place = lax.broadcasted_iota(jnp.int32, (seq, rows), 0)
    spans = [slice(e * seq, (e + 1) * seq) for e in range(examples)]
    live = [place < counts_ref[e] for e in range(examples)]
    hidden = acc_x[:, :rank].astype(jnp.bfloat16)
    rank_ref[...] = dot32(hidden, rb_ref[...], NN).astype(jnp.bfloat16)

    @pl.loop(0, chunks)
    def _(c):
        for move in g_moves(c):
            move.wait()
        weights = jnp.concatenate([b_ref[span_of(c), :], of_ref[c].T], axis=1)
        acc_g[...] += dot32(g_ref[c], weights, NN)

    back = acc_g[:, :rank].astype(jnp.bfloat16)
    back_rank = dot32(back, ra_ref[...], NN).astype(jnp.bfloat16)
    for e, span in enumerate(spans):
        gp = jnp.where(live[e], acc_g[span, rank:], 0.0).astype(jnp.bfloat16)
        ip = jnp.where(live[e], acc_x[span, rank:], 0.0).astype(jnp.bfloat16)
        term = dot32(gp, rank_ref[span, :], TN) + dot32(ip, back_rank[span], TN)
        term = (term / counts_ref[e].astype(jnp.float32)).astype(jnp.bfloat16)
        for f in range(feat_size):
            for q in range(copies):
                out_ref[f, q, e] = term[f * part : (f + 1) * part]


def project(counts, arrays, feat_size, copies, examples):
    x, _, a, _, of_t, _, rb, _ = arrays
    tokens, width = x.shape
    rank, rows = a.shape[0], of_t.shape[0]
    chunk = width // CHUNKS
    out = (feat_size, copies, examples, rows // feat_size, rb.shape[1])
    hbm = pl.BlockSpec(memory_space=pltpu.HBM)
    vmem = pl.BlockSpec(memory_space=pltpu.VMEM)
    fixed = [
        pltpu.with_memory_space_constraint(array, pltpu.HBM) if n not in (2, 3) else array
        for n, array in enumerate(arrays)
    ]
    low = [
        (CHUNKS, tokens, chunk),
        (CHUNKS, tokens, chunk),
        (CHUNKS, rows, chunk),
        (CHUNKS, rows, chunk),
        rb.shape,
        rb.shape,
    ]
    return pl.pallas_call(
        project_kernel,
        in_specs=[pl.BlockSpec(memory_space=pltpu.SMEM)] + [hbm] * 2 + [vmem] * 2 + [hbm] * 4,
        out_specs=vmem,
        out_shape=pltpu.VMEM(out, jnp.bfloat16),
        scratch_shapes=[pltpu.VMEM(shape, jnp.bfloat16) for shape in low]
        + [
            pltpu.VMEM((tokens, rank + rows), jnp.float32),
            pltpu.VMEM((tokens, rank + rows), jnp.float32),
            pltpu.VMEM((tokens, rb.shape[1]), jnp.bfloat16),
            pltpu.SemaphoreType.DMA((CHUNKS, 2)),
            pltpu.SemaphoreType.DMA((CHUNKS, 2)),
            pltpu.SemaphoreType.DMA((2,)),
        ],
        cost_estimate=pl.CostEstimate(
            flops=4 * tokens * width * (rank + rows),
            bytes_accessed=2 * (2 * tokens + 2 * rank + 2 * rows) * width,
            transcendentals=0,
        ),
        compiler_params=pltpu.CompilerParams(vmem_limit_bytes=PROJECT_VMEM),
        name="project",
    )(counts, *fixed)


def combine_kernel(index_ref, parts_ref, *rest):
    pieces = rest[:-4]
    feat_ref, pack_ref, summed, flat = rest[-4:]
    feat_size, copies, examples, part, cols = parts_ref.shape
    width = part * cols
    members = copies * examples
    total = parts_ref[0].astype(jnp.float32)
    for f in range(1, feat_size):
        total = total + parts_ref[f].astype(jnp.float32)
    summed[...] = total.reshape(members * part, cols)
    flat[...] = jnp.zeros_like(flat)
    mine = index_ref[0] * (examples * part)
    for k in range(part):
        span = slice(k * cols, (k + 1) * cols)
        flat[:members, span] = summed[pl.ds(k, members, stride=part), :]
        feat_ref[:, span] = summed[pl.ds(mine + k, examples, stride=part), :].astype(jnp.bfloat16)
    features = flat[...].astype(jnp.bfloat16)
    rounded = features.astype(jnp.float32)
    norm = jnp.sum(rounded * rounded, axis=1, keepdims=True)
    vals = jnp.concatenate([ref[:, :width] for ref in pieces], axis=0)
    count = vals.shape[0]
    rows = pieces[0].shape[0]
    inner = dot32(features, vals, NT)
    squares = jnp.zeros((count, LANES), jnp.float32)
    for c in range(0, width, LANES):
        piece = vals[:, c : c + LANES].astype(jnp.float32)
        squares = squares + piece * piece
    val_norm = dot32(jnp.ones((SUBLANES, LANES), jnp.float32), squares, NT, HIGHEST)
    ids = jnp.concatenate(
        [ref[:SUBLANES, width : width + rows].astype(jnp.float32) for ref in pieces], axis=1
    )
    pack_ref[...] = jnp.full(pack_ref.shape, -1.0, jnp.float32)
    lanes = pack_ref.shape[-1]
    for q in range(copies):
        span = slice(q * examples, (q + 1) * examples)
        wide = jnp.broadcast_to(norm[span], (examples, lanes))
        for f in range(feat_size):
            pack_ref[f, q, :examples, :count] = inner[span]
            pack_ref[f, q, examples : 2 * examples, :] = wide
            pack_ref[f, q, 2 * examples : 2 * examples + 1, :count] = val_norm[:1]
            pack_ref[f, q, 2 * examples + 1 : 2 * examples + 2, :count] = ids[:1]


def score_kernel(count, scale, packs_ref, held_ref, out_ref, feat_ref):
    feat_ref[...] = held_ref[...]
    feat_size, copies, _, _ = packs_ref.shape
    examples = out_ref.shape[0]
    total = packs_ref[0]
    for f in range(1, feat_size):
        total = total + packs_ref[f]
    inner = total[:, :examples, :count]
    norm = total[0, examples : 2 * examples, :count]
    val_norm = total[:, 2 * examples : 2 * examples + 1, :count]
    ids = packs_ref[0, :, 2 * examples + 1 : 2 * examples + 2, :count]
    root = lax.rsqrt(norm + norm_eps)
    sums = jnp.zeros((examples, DOMAINS), jnp.float32)
    sizes = jnp.zeros((examples, DOMAINS), jnp.float32)
    ones = jnp.ones((examples, count), jnp.float32)
    domain = lax.broadcasted_iota(jnp.int32, (DOMAINS, count), 0).astype(jnp.float32)
    for q in range(copies):
        cosine = inner[q] * root * lax.rsqrt(val_norm[q] + norm_eps)
        marks = jnp.where(jnp.broadcast_to(ids[q], domain.shape) == domain, 1.0, 0.0)
        sums = sums + dot32(cosine, marks, NT, HIGHEST)
        sizes = sizes + dot32(ones, marks, NT)
    out_ref[...] = scale * sums / sizes


def axis_count(sizes, names):
    total = 1
    for name in names:
        total *= sizes[name]
    return total


def local(
    sizes,
    layer_inputs,
    output_grads,
    adapter_a,
    adapter_b,
    out_factor,
    in_factor,
    rank_factor_b,
    rank_factor_a,
    token_counts,
    val_grads,
    val_domain,
):
    _, examples, seq_len, width = layer_inputs.shape
    val_rows, val_cols = val_grads.shape
    feat_size = sizes["feat"]
    copies = axis_count(sizes, NEAR)
    far_size = axis_count(sizes, FAR)

    payload = pl.pallas_call(
        payload_kernel,
        in_specs=[pl.BlockSpec(memory_space=pltpu.HBM)] * 2,
        out_specs=pl.BlockSpec(memory_space=pltpu.VMEM),
        out_shape=pltpu.VMEM((val_rows, val_cols + LANES), jnp.bfloat16),
        scratch_shapes=[
            pltpu.VMEM((1, val_rows), jnp.int32),
            pltpu.SemaphoreType.DMA((2,)),
        ],
        cost_estimate=pl.CostEstimate(
            flops=8_000_000_000, bytes_accessed=16_000_000, transcendentals=0
        ),
        compiler_params=limit(4),
        name="payload",
    )(
        pltpu.with_memory_space_constraint(val_grads, pltpu.HBM),
        pltpu.with_memory_space_constraint(val_domain.T, pltpu.HBM),
    )
    pieces = [payload]
    power = far_size & (far_size - 1) == 0
    for s in range(far_size - 1, 0, -1):
        pairs = [(i, i ^ s if power else (i + s) % far_size) for i in range(far_size)]
        pieces.append(lax.ppermute(payload, FAR, pairs))

    arrays = (
        layer_inputs.reshape(examples * seq_len, width),
        output_grads.reshape(examples * seq_len, width),
        adapter_a[0],
        adapter_b[0],
        out_factor[0].T,
        in_factor[0].T,
        rank_factor_b[0],
        rank_factor_a[0],
    )
    parts = project(token_counts, arrays, feat_size, copies, examples)
    group = ("feat",) + NEAR
    members = feat_size * copies
    index = lax.axis_index(NEAR).astype(jnp.int32).reshape(1)
    parts, index = lax.optimization_barrier((parts, index))
    flat_parts = parts.reshape((members,) + parts.shape[2:])
    got = lax.all_to_all(flat_parts, group, 0, 0, tiled=True).reshape(parts.shape)

    count = far_size * val_rows
    lanes = round_up(count, LANES)
    block_rows = round_up(2 * examples + 2, SUBLANES)
    part, cols = parts.shape[3:]
    smem = pl.BlockSpec(memory_space=pltpu.SMEM)
    vmem = pl.BlockSpec(memory_space=pltpu.VMEM)
    held, packs = pl.pallas_call(
        combine_kernel,
        in_specs=[smem] + [vmem] * (1 + far_size),
        out_shape=[
            pltpu.VMEM((examples, val_cols), jnp.bfloat16),
            pltpu.VMEM((feat_size, copies, block_rows, lanes), jnp.float32),
        ],
        scratch_shapes=[
            pltpu.VMEM((copies * examples * part, cols), jnp.float32),
            pltpu.VMEM((round_up(copies * examples, 2 * SUBLANES), val_cols), jnp.float32),
        ],
        compiler_params=limit(8),
        name="combine",
    )(index, got, *pieces)

    flat_packs = packs.reshape((members,) + packs.shape[2:])
    returned = lax.all_to_all(flat_packs, group, 0, 0, tiled=True).reshape(packs.shape)
    domain_scores, train_features = pl.pallas_call(
        functools.partial(score_kernel, count, math.sqrt(PROJ)),
        out_shape=[
            jax.ShapeDtypeStruct((examples, DOMAINS), jnp.float32),
            jax.ShapeDtypeStruct((examples, val_cols), jnp.bfloat16),
        ],
        compiler_params=limit(4),
        name="score",
    )(returned, held)
    return (train_features, domain_scores)


def solution(mesh):
    in_specs = (
        P("feat", DP, None, None),
        P("feat", DP, None, None),
        P("feat", None, None),
        P("feat", None, None),
        P("feat", None, None),
        P("feat", None, None),
        P("feat", None, None),
        P("feat", None, None),
        P(DP),
        P(DP, "feat"),
        P(DP, None),
    )
    out_specs = (P(DP, "feat"), P(DP, None))
    feat_size, dp_size = mesh.shape["feat"], mesh.shape["dp"]
    sizes = {"feat": feat_size, "hi": dp_size // 4, "lo": 2, "core": 2}
    split = Mesh(mesh.devices.reshape(tuple(sizes.values())), tuple(sizes))
    body = functools.partial(local, sizes)
    return jax.shard_map(body, mesh=split, in_specs=in_specs, out_specs=out_specs, check_vma=False)
```
